32 devices in a mesh: dp: 4 (over y, x), vocab: 8 (over z, core).
Axes of the slice: x: 2, y: 2, z: 4, core: 2. Of those that a mesh axis runs over, the one named last changes fastest.
Arguments:
- hidden: bfloat16 [1024, 8192], P('dp'), may hold values from -14 to 14
- weight: bfloat16 [8192, 8192], P('dp', 'vocab'), may hold values from -1 to 1, as said below
- targets: int32 [1024], P('dp'), may hold values from 0 to 8191
- cotangent: float32 [1024], P('dp'), may hold values from 1 to 8
Outputs:
- loss: float32 [1024], P('dp')
- grad_hidden: bfloat16 [1024, 8192], P('vocab', 'dp')
- grad_weight: bfloat16 [8192, 8192], P('dp', 'vocab')
The draws below stay inside these ranges and needn't reach their ends.
Inputs may be any that keep to these rules, and one draw needn't show every extreme that they name: `weight`: entries drawn with standard deviation 4 / sqrt(8192).
All inputs are finite; a program needn't handle non-finite values.
Results may differ from the reference program's by a relative error of at most 0.0047.
Values may be sent and summed in bfloat16 or wider, within the bound.
A program may use at most 128 MiB of HBM per device.

```python
import math
import jax
import jax.numpy as jnp
from jax import lax

D = 8192
VOCAB = 8192
TOKENS = 1024


def joint_draw(key):
    weight_key = jax.random.fold_in(key, 11)
    hidden_key = jax.random.fold_in(key, 12)
    weight = jnp.clip(jnp.clip(jax.random.normal(weight_key, (D, VOCAB), jnp.float32), -6.0, 6.0) * (4.0 / D ** 0.5), -1.0, 1.0)
    hidden = jnp.clip(jax.random.normal(hidden_key, (TOKENS, D), jnp.float32), -6.0, 6.0)
    return (weight, hidden)


def draw_weight(key, part):
    weight, hidden = joint_draw(key)
    return weight.astype(jnp.bfloat16)


def draw_hidden(key, part):
    weight, hidden = joint_draw(key)
    return hidden.astype(jnp.bfloat16)


def set_ends(result, key, smallest, top_value):
    longest = result.shape.index(max(result.shape))
    spots = []
    for shift in (0, 1):
        where = [jax.random.randint(jax.random.fold_in(key, axis), (), 0, length) for axis, length in enumerate(result.shape)]
        where[longest] = (where[longest] + shift) % result.shape[longest]
        spots.append(tuple(where))
    return result.at[spots[0]].set(smallest).at[spots[1]].set(top_value)


def shard_levels(own_key, dims, split, smallest, top_value):
    def one(position, shards_of):
        steps = jax.random.uniform(jax.random.fold_in(jax.random.fold_in(own_key, 6), position), (shards_of,), jnp.float32, smallest / len(split), top_value / len(split))
        return jnp.repeat(jnp.exp(steps), dims[position] // shards_of).reshape((-1,) + (1,) * (len(dims) - position - 1))

    gain = one(*split[0])
    for cut in split[1:]:
        gain = gain * one(*cut)
    return gain


def setup_inputs(seed: int = 0) -> dict:
    key_list = jax.random.split(jax.random.key(seed), 5)
    return {
        "hidden": draw_hidden(jax.random.fold_in(key_list[4], 71), 0),
        "weight": draw_weight(jax.random.fold_in(key_list[4], 71), 0),
        "targets": set_ends(jax.random.randint(key_list[2], (TOKENS,), 0, VOCAB), jax.random.fold_in(key_list[2], 1), 0, VOCAB - 1).astype(jnp.int32),
        "cotangent": jnp.clip(jnp.exp(math.log(8.0) - 2.0794415 * jax.random.uniform(key_list[3], (TOKENS,), jnp.float32) ** shard_levels(key_list[3], (TOKENS,), ((0, 4),), -0.2, 0.2)), 1.0, 8.0),
    }


def reference(hidden, weight, targets, cotangent):
    logits = jnp.dot(hidden, weight, preferred_element_type=jnp.float32)
    row_max = jnp.max(logits, axis=1, keepdims=True)
    shifted = jnp.exp(logits - row_max)
    sum_exp = jnp.sum(shifted, axis=1, keepdims=True)
    columns = jnp.arange(VOCAB, dtype=jnp.int32)
    onehot = (targets.astype(jnp.int32)[:, None] == columns[None, :]).astype(jnp.float32)
    picked = jnp.sum(logits * onehot, axis=1)
    loss = row_max[:, 0] + jnp.log(sum_exp[:, 0]) - picked
    grad_logits = (cotangent[:, None] * (shifted / sum_exp - onehot)).astype(jnp.bfloat16)
    grad_hidden = lax.dot_general(grad_logits, weight, (((1,), (1,)), ((), ())), preferred_element_type=jnp.float32).astype(jnp.bfloat16)
    grad_weight = lax.dot_general(hidden, grad_logits, (((0,), (0,)), ((), ())), preferred_element_type=jnp.float32).astype(jnp.bfloat16)
    return (loss, grad_hidden, grad_weight)
```

```python
import functools

import jax
import jax.numpy as jnp
from jax import lax
from jax.experimental import pallas as pl
from jax.experimental.pallas import tpu as pltpu
from jax.sharding import PartitionSpec as P

F32 = jnp.float32
BF16 = jnp.bfloat16
WIRE = jnp.int16
STEPS = 32000.0


def butterfly_kernel(
    nd, nv, levels,
    h_ref, w_hbm, t_ref, c_ref,
    loss_ref, gh_ref, gw_ref,
    w, spread, logit, psend, precv, stats, grads, acc, sbuf, rbuf, gwbuf, tcol, ccol, col,
    part_f32, usend, urecv, ucol,
    w_sem, own_sem, gw_sem,
    hs_send, hs_recv, hf_send, hf_recv, hx_send, hx_recv, p_send, p_recv, u_send, u_recv,
    st_send, st_recv, g_send, g_recv, x_send, x_recv, r_send, r_recv,
):
    d, v = lax.axis_index("dp"), lax.axis_index("vocab")
    core = lax.rem(v, 2)

    def flip(i, mask):
        for bit in range(mask.bit_length()):
            if mask >> bit & 1:
                i = i + (1 - 2 * lax.rem(i // (1 << bit), 2)) * (1 << bit)
        return i

    mate, across = flip(v, 1), flip(v, 2)
    side = lax.rem(v // 2, 2)
    depth, width = w.shape
    tokens = spread.shape[0]
    rows = tokens // nd
    half = rows // 2
    quarter = rows // 4
    share = tokens // nv
    per = rows // share

    load_w = pltpu.make_async_copy(w_hbm, w, w_sem)
    load_w.start()
    own_rows = pl.ds(pl.multiple_of(d * rows, rows), rows)
    load_own = pltpu.make_async_copy(
        h_ref.at[:, pl.ds(pl.multiple_of(d * depth, depth), depth)], spread.at[own_rows], own_sem
    )
    load_own.start()

    barrier = pltpu.get_barrier_semaphore()
    for k in range(1, nd):
        pl.semaphore_signal(barrier, inc=1, device_id={"dp": flip(d, k)})
    for k in range(1, nv):
        pl.semaphore_signal(barrier, inc=1, device_id={"vocab": lax.rem(v + k, nv)})
    pl.semaphore_wait(barrier, nd + nv - 2)

    def remote(src, dst, send, recv, where):
        return pltpu.make_async_remote_copy(
            src_ref=src, dst_ref=dst, send_sem=send, recv_sem=recv, device_id=where
        )

    def piece(s, q):
        return spread.at[pl.ds(pl.multiple_of(s * rows + q * quarter, quarter), quarter)]

    mine = 2 * side + core
    hidden_sends = []
    for k in range(1, nd):
        to = flip(d, k)
        copy = remote(
            h_ref.at[
                pl.ds(pl.multiple_of(mine * quarter, quarter), quarter),
                pl.ds(pl.multiple_of(to * depth, depth), depth),
            ],
            piece(d, mine), hs_send.at[k - 1], hs_recv.at[k - 1], {"dp": to},
        )
        copy.start()
        hidden_sends.append(copy)

    tcol[...] = jnp.broadcast_to(t_ref[...], (128, rows)).T
    ccol[...] = jnp.broadcast_to(c_ref[...], (128, rows)).T

    tile = min(256, width)
    code_rows = min(32, half)

    def project(first, count, store):
        def step(n, _):
            cols = pl.ds(pl.multiple_of(n * tile, tile), tile)
            store(cols, jnp.dot(
                spread[pl.ds(pl.multiple_of(first, count), count), :], w[:, cols],
                preferred_element_type=F32,
            ))
            return 0

        lax.fori_loop(0, width // tile, step, 0)

    load_w.wait()
    load_own.wait()

    def store_own(cols, value):
        logit[:, cols] = value

    project(d * rows, rows, store_own)

    forwards, crossings, partial_sends = [], [], []
    for turn in range(2):
        for k in range(1, nd):
            s = flip(d, k)
            part = side if turn == 0 else 1 - side
            got = piece(s, 2 * part + core)
            to_mate = remote(got, got, hf_send.at[k - 1, turn], hf_recv.at[k - 1, turn], {"vocab": mate})
            over = remote(got, got, hx_send.at[k - 1], hx_recv.at[k - 1], {"vocab": across})
            if turn == 0:
                remote(got, got, hs_send.at[k - 1], hs_recv.at[k - 1], {"dp": s}).wait_recv()
                over.start()
                crossings.append(over)
            else:
                over.wait_recv()
            to_mate.start()
            forwards.append(to_mate)
            to_mate.wait_recv()
            there = pl.ds(pl.multiple_of(part * half, half), half)

            def store_part(cols, value):
                part_f32[:, cols] = value

            project(s * rows + part * half, half, store_part)

            def encode(i, _, k=k, part=part):
                at = pl.ds(pl.multiple_of(i * code_rows, code_rows), code_rows)
                x = part_f32[at, :]
                unit = jnp.maximum(jnp.max(jnp.abs(x), axis=1, keepdims=True), 1e-30) / STEPS
                there = pl.ds(pl.multiple_of(part * half + i * code_rows, code_rows), code_rows)
                psend[k - 1, there, :] = jnp.round(x / unit).astype(jnp.int32).astype(WIRE)
                col[at, :] = jnp.broadcast_to(unit, (code_rows, 128))
                return 0

            lax.fori_loop(0, half // code_rows, encode, 0)
            usend[k - 1, turn] = col[:half, :].T[:8, :]
            for copy in (
                remote(
                    psend.at[k - 1, there], precv.at[k - 1, there],
                    p_send.at[k - 1, turn], p_recv.at[k - 1, turn], {"dp": s},
                ),
                remote(
                    usend.at[k - 1, turn], urecv.at[k - 1, turn],
                    u_send.at[k - 1, turn], u_recv.at[k - 1, turn], {"dp": s},
                ),
            ):
                copy.start()
                partial_sends.append(copy)
    for copy in partial_sends:
        copy.wait_recv()
    for k in range(1, nd):
        for turn in range(2):
            part = side if turn == 0 else 1 - side
            there = pl.ds(pl.multiple_of(part * half, half), half)
            ucol[k - 1, there, :] = jnp.broadcast_to(urecv[k - 1, turn][0:1, :], (128, half)).T

    step_rows = min(32, rows)
    column = lax.broadcasted_iota(jnp.int32, (step_rows, width), 1) + v * width
    lane = lax.broadcasted_iota(jnp.int32, (step_rows, 128), 1)

    def measure(i, _):
        at = pl.ds(pl.multiple_of(i * step_rows, step_rows), step_rows)
        x = logit[at, :]
        for k in range(1, nd):
            x = x + precv[k - 1, at, :].astype(jnp.int32).astype(F32) * ucol[k - 1, at, :1]
        top = jnp.max(x, axis=1, keepdims=True)
        e = jnp.exp(x - top)
        total = jnp.sum(e, axis=1, keepdims=True)
        pick = jnp.sum(jnp.where(column == tcol[at, :1], x, 0.0), axis=1, keepdims=True)
        logit[at, :] = e
        col[at, :] = jnp.where(lane == 0, top, jnp.where(lane == 1, total, pick))
        return 0

    lax.fori_loop(0, rows // step_rows, measure, 0)
    stats[v] = col[...].T[:8, :]
    stat_sends = []
    for k in range(1, nv):
        copy = remote(
            stats.at[v], stats.at[v], st_send.at[k - 1], st_recv.at[k - 1],
            {"vocab": lax.rem(v + k, nv)},
        )
        copy.start()
        stat_sends.append(copy)
    own_top = stats[v][0:1, :]
    for copy in stat_sends:
        copy.wait_recv()
    top = stats[0][0:1, :]
    for u in range(1, nv):
        top = jnp.maximum(top, stats[u][0:1, :])
    total = jnp.zeros_like(top)
    pick = jnp.zeros_like(top)
    for u in range(nv):
        block = stats[u]
        total = total + block[1:2, :] * jnp.exp(block[0:1, :] - top)
        pick = pick + block[2:3, :]
    loss_ref[...] = top + jnp.log(total) - pick
    scale = c_ref[...] * jnp.exp(own_top - top) / total
    col[...] = jnp.broadcast_to(scale, (128, rows)).T

    def differentiate(i, _):
        at = pl.ds(pl.multiple_of(i * step_rows, step_rows), step_rows)
        onehot = jnp.where(column == tcol[at, :1], ccol[at, :1], 0.0)
        g = logit[at, :] * col[at, :1] - onehot
        grads[pl.ds(pl.multiple_of(d * rows + i * step_rows, step_rows), step_rows), :] = g.astype(BF16)
        return 0

    lax.fori_loop(0, rows // step_rows, differentiate, 0)
    relayed = nd == 4
    grad_sends = []
    for k in range(1, nd - 1 if relayed else nd):
        copy = remote(
            grads.at[own_rows], grads.at[own_rows], g_send.at[k - 1], g_recv.at[k - 1],
            {"dp": flip(d, k)},
        )
        copy.start()
        grad_sends.append(copy)

    def relay(k):
        block = grads.at[pl.ds(pl.multiple_of(flip(d, k) * rows + (k - 1) * half, half), half)]
        return remote(block, block, x_send.at[k - 1], x_recv.at[k - 1], {"dp": flip(d, 3 - k)})

    relays = [relay(1), relay(2)] if relayed else []

    depth_tile = min(256, depth)

    def pull(k):
        s = flip(d, k)

        def step(n, _):
            at = pl.ds(pl.multiple_of(n * depth_tile, depth_tile), depth_tile)
            value = lax.dot_general(
                grads[pl.ds(pl.multiple_of(s * rows, rows), rows), :], w[at, :],
                (((1,), (1,)), ((), ())), preferred_element_type=F32,
            )
            for j in range(per):
                acc[k * per + j, :, at] = value[j * share:(j + 1) * share, :]
            return 0

        lax.fori_loop(0, depth // depth_tile, step, 0)

    def ahead(b):
        s = flip(d, b // per)
        return s * per + b % per - v + nv

    def partner(level):
        bit = lax.rem(v // (1 << level), 2)
        return {"vocab": v + (1 - 2 * bit) * (1 << level)}

    chunk = min(16, share)

    cuts = 2
    span = depth // cuts

    def hop(b, level, q):
        at = pl.ds(q * span, span)
        return remote(
            sbuf.at[b, :, at], rbuf.at[level, b, :, at], r_send.at[b, q], r_recv.at[level, b, q], partner(level)
        )

    def each_chunk(body):
        def step(i, _):
            body(pl.ds(pl.multiple_of(i * chunk, chunk), chunk))
            return 0

        lax.fori_loop(0, share // chunk, step, 0)

    def send(b, level, q):
        mine = lax.rem(ahead(b), 1 << level) == 0
        leaves = lax.rem(ahead(b), 2 << level) != 0
        cols = pl.ds(q * span, span)

        @pl.when(jnp.logical_and(mine, leaves))
        def _():
            def body(at):
                sbuf[b, at, cols] = acc[b, at, cols].astype(BF16)

            each_chunk(body)
            hop(b, level, q).start()

    def receive(b, level):
        for q in range(cuts):
            cols = pl.ds(q * span, span)

            @pl.when(lax.rem(ahead(b), 2 << level) == 0)
            def _(q=q, cols=cols):
                hop(b, level, q).wait_recv()

                def body(at):
                    acc[b, at, cols] = acc[b, at, cols] + rbuf[level, b, at, cols].astype(F32)

                each_chunk(body)

            if level + 1 < levels:
                send(b, level + 1, q)

    def arrive(k):
        if relayed and k == nd - 1:
            for copy in relays:
                copy.wait_recv()
        elif k:
            grad_sends[k - 1].wait_recv()
            if relayed:
                relays[k - 1].start()

    pending = []
    for k in range(nd):
        if relayed and k == 1:
            arrive(1)
            arrive(2)
        elif not (relayed and k == 2):
            arrive(k)
        pull(k)
        for j in range(per):
            for q in range(cuts):
                send(k * per + j, 0, q)
        for j in range(per):
            receive(k * per + j, 0)
            pending.append(k * per + j)
        if k >= 2 and levels > 1:
            for b in pending[:per]:
                receive(b, 1)
            pending = pending[per:]

    def weigh(n, _):
        at = pl.ds(pl.multiple_of(n * depth_tile, depth_tile), depth_tile)
        gwbuf[at, :] = lax.dot_general(
            spread[:, at], grads[...], (((0,), (0,)), ((), ())), preferred_element_type=F32
        ).astype(BF16)
        pltpu.make_async_copy(gwbuf.at[at], gw_ref.at[at], gw_sem.at[n]).start()
        return 0

    lax.fori_loop(0, depth // depth_tile, weigh, 0)

    for level in range(1, levels):
        for b in pending if level == 1 else range(nv):
            receive(b, level)
    for b in range(nv):
        @pl.when(ahead(b) == nv)
        def _(b=b):
            def body(at):
                gh_ref[at, :] = acc[b, at, :].astype(BF16)

            each_chunk(body)

        @pl.when(ahead(b) != nv)
        def _(b=b):
            for q in range(cuts):
                hop(b, 0, q).wait_send()

    for copy in hidden_sends + forwards + crossings + partial_sends + stat_sends + grad_sends + relays:
        copy.wait_send()
    for n in range(depth // depth_tile):
        at = pl.ds(n * depth_tile, depth_tile)
        pltpu.make_async_copy(gwbuf.at[at], gw_ref.at[at], gw_sem.at[n]).wait()


def butterfly(nd, nv, hidden, weight, targets, cotangent):
    rows = hidden.shape[0]
    tokens = rows * nd
    depth, width = weight.shape
    share = tokens // nv
    levels = nv.bit_length() - 1
    dma = pltpu.SemaphoreType.DMA
    vmem = pl.BlockSpec(memory_space=pltpu.VMEM)
    anywhere = pl.BlockSpec(memory_space=pl.ANY)
    flops = 6 * tokens * depth * width
    loss, grad_hidden, grad_weight = pl.pallas_call(
        functools.partial(butterfly_kernel, nd, nv, levels),
        out_shape=(
            jax.ShapeDtypeStruct((1, rows), F32),
            jax.ShapeDtypeStruct((share, depth), BF16),
            jax.ShapeDtypeStruct((depth, width), BF16),
        ),
        in_specs=[anywhere, anywhere, vmem, vmem],
        out_specs=(vmem, vmem, anywhere),
        scratch_shapes=[
            pltpu.VMEM((depth, width), BF16),
            pltpu.VMEM((tokens, depth), BF16),
            pltpu.VMEM((rows, width), F32),
            pltpu.VMEM((nd - 1, rows, width), WIRE),
            pltpu.VMEM((nd - 1, rows, width), WIRE),
            pltpu.VMEM((nv, 8, rows), F32),
            pltpu.VMEM((tokens, width), BF16),
            pltpu.VMEM((nv, share, depth), F32),
            pltpu.VMEM((nv, share, depth), BF16),
            pltpu.VMEM((levels, nv, share, depth), BF16),
            pltpu.VMEM((depth, width), BF16),
            pltpu.VMEM((rows, 128), jnp.int32),
            pltpu.VMEM((rows, 128), F32),
            pltpu.VMEM((rows, 128), F32),
            pltpu.VMEM((rows // 2, width), F32),
            pltpu.VMEM((nd - 1, 2, 8, rows // 2), F32),
            pltpu.VMEM((nd - 1, 2, 8, rows // 2), F32),
            pltpu.VMEM((nd - 1, rows, 128), F32),
            dma, dma, dma((depth // min(256, depth),)),
            dma((nd - 1,)), dma((nd - 1,)), dma((nd - 1, 2)), dma((nd - 1, 2)), dma((nd - 1,)), dma((nd - 1,)),
            dma((nd - 1, 2)), dma((nd - 1, 2)), dma((nd - 1, 2)), dma((nd - 1, 2)),
            dma((nv - 1,)), dma((nv - 1,)),
            dma((nd - 1,)), dma((nd - 1,)),
            dma((2,)), dma((2,)),
            dma((nv, 2)), dma((levels, nv, 2)),
        ],
        compiler_params=pltpu.CompilerParams(
            collective_id=0, has_side_effects=True, vmem_limit_bytes=66_000_000
        ),
        cost_estimate=pl.CostEstimate(flops=flops, bytes_accessed=16 << 20, transcendentals=0),
        name="token_loss",
    )(hidden, weight, targets.reshape(1, rows), cotangent.reshape(1, rows))
    return loss.reshape(rows), grad_hidden, grad_weight


CHUNKS = 4
VMEM_GRANT = 58_000_000


def chain_kernel(
    nd, nv, plan,
    h_ref, w_hbm, t_ref, c_ref,
    loss_ref, gh_ref, gw_ref,
    w, spread, part, psend, precv, usend, urecv, stats, grads, acc, xsend, xrecv, zsend, zrecv,
    tcol, ccol, col, losscol,
    w_sem, own_sem,
    hs_send, hs_recv, hx_send, hx_recv, hf_send, hf_recv, p_send, p_recv, u_send, u_recv,
    st_send, st_recv, g_send, g_recv, r_send, r_recv, x_send, x_recv, z_send, z_recv,
):
    d, v = lax.axis_index("dp"), lax.axis_index("vocab")
    z, core = v // 2, lax.rem(v, 2)
    chips = nv // 2
    side = lax.rem(z, 2)
    depth, width = w.shape
    chunks, _, count, _ = spread.shape
    rows = tcol.shape[0]
    half = rows // 2
    cr = count // 2
    qr = count // 4
    total_rows = nd * count

    def flip(i, mask):
        for bit in range(mask.bit_length()):
            if mask >> bit & 1:
                i = i + (1 - 2 * lax.rem(i // (1 << bit), 2)) * (1 << bit)
        return i

    def xor(a, b):
        return lax.rem(a + b, 2) + 2 * lax.rem(a // 2 + b // 2, 2)

    mate, across = flip(v, 1), flip(v, 2)

    def remote(src, dst, send, recv, where):
        return pltpu.make_async_remote_copy(
            src_ref=src, dst_ref=dst, send_sem=send, recv_sem=recv, device_id=where
        )

    load_w = pltpu.make_async_copy(w_hbm, w, w_sem)
    load_w.start()
    own_cols = pl.ds(pl.multiple_of(d * depth, depth), depth)

    def own_load(c, h):
        return pltpu.make_async_copy(
            h_ref.at[pl.ds(h * half + c * cr, cr), own_cols],
            spread.at[c, 0, pl.ds(h * cr, cr)], own_sem.at[c, h],
        )

    for c in range(chunks):
        for h in range(2):
            own_load(c, h).start()

    barrier = pltpu.get_barrier_semaphore()
    for k in range(1, nd):
        pl.semaphore_signal(barrier, inc=1, device_id={"dp": flip(d, k)})
    for k in range(1, nv):
        pl.semaphore_signal(barrier, inc=1, device_id={"vocab": lax.rem(v + k, nv)})
    pl.semaphore_wait(barrier, nd + nv - 2)

    sent = []

    def go(copy):
        copy.start()
        sent.append(copy)

    def hidden_copy(c, k):
        to = flip(d, k)
        first = pl.multiple_of(side * half + c * cr + core * qr, qr)
        return remote(
            h_ref.at[pl.ds(first, qr), pl.ds(pl.multiple_of(to * depth, depth), depth)],
            spread.at[c, k, pl.ds(pl.multiple_of((2 * side + core) * qr, qr), qr)],
            hs_send.at[c, k - 1], hs_recv.at[c, k - 1], {"dp": to},
        )

    def slab(c, piece):
        return spread.at[c, pl.ds(1, nd - 1), pl.ds(pl.multiple_of(piece * qr, qr), qr)]

    def across_copy(c):
        block = slab(c, 2 * side + core)
        return remote(block, block, hx_send.at[c], hx_recv.at[c], {"vocab": across})

    def mate_copy(c, turn):
        block = slab(c, 2 * (side if turn == 0 else 1 - side) + core)
        return remote(block, block, hf_send.at[c, turn], hf_recv.at[c, turn], {"vocab": mate})

    for c in range(chunks):
        for k in (3, 1, 2):
            go(hidden_copy(c, k))

    tcol[...] = jnp.broadcast_to(t_ref[...], (128, rows)).T
    ccol[...] = jnp.broadcast_to(c_ref[...], (128, rows)).T
    load_w.wait()

    def gather(c):
        for k in range(1, nd):
            hidden_copy(c, k).wait_recv()
        go(across_copy(c))
        go(mate_copy(c, 0))

    def cross(c):
        across_copy(c).wait_recv()
        go(mate_copy(c, 1))

    tile = min(256, width)

    def project(c):
        for h in range(2):
            own_load(c, h).wait()
        for turn in range(2):
            mate_copy(c, turn).wait_recv()

        def step(n, _):
            cols = pl.ds(pl.multiple_of(n * tile, tile), tile)
            value = jnp.dot(
                spread[c].reshape(total_rows, depth), w[:, cols], preferred_element_type=F32
            )
            part[c, :, :, cols] = value.reshape(nd, count, tile)
            return 0

        lax.fori_loop(0, width // tile, step, 0)

    def encode(c, k, h, x):
        at = pl.ds(h * cr, cr)
        top = jnp.maximum(jnp.max(jnp.abs(x), axis=1, keepdims=True), 1e-30)
        psend[c, k - 1, at, :] = jnp.round(x * (STEPS / top)).astype(jnp.int32).astype(WIRE)
        col[c, k - 1, at, :] = jnp.broadcast_to(top / STEPS, (cr, 128))

    def part_copy(c, k, h, to, n):
        at = pl.ds(h * cr, cr)
        return remote(
            psend.at[c, k - 1, at], precv.at[c, k - 1, at], p_send.at[c, n], p_recv.at[c, n], {"dp": flip(d, to)}
        )

    def unit_copy(c, k, n):
        to = (1, 2, 1, 2)[n]
        return remote(
            usend.at[c, k - 1], urecv.at[c, n], u_send.at[c, n], u_recv.at[c, n], {"dp": flip(d, to)}
        )

    def scatter(c):
        for h in range(2):
            encode(c, 3, h, part[c, 3, h * cr:(h + 1) * cr, :])
        usend[c, 2] = col[c, 2].T[:8, :]
        for h in range(2):
            go(part_copy(c, 3, h, h + 1, h))
            go(unit_copy(c, 3, h))
        for k in (1, 2):
            h = k - 1
            encode(c, k, h, part[c, k, h * cr:(h + 1) * cr, :])
            go(part_copy(c, k, h, k, 1 + k))

    def combine(c):
        for h in range(2):
            part_copy(c, 3, h, h + 1, h).wait_recv()
            unit_copy(c, 3, h).wait_recv()
        lane = lax.broadcasted_iota(jnp.int32, (1, count), 1)
        unit = jnp.where(lane < cr, urecv[c, 0][0:1, :], urecv[c, 1][0:1, :])
        ucol = jnp.broadcast_to(unit, (128, count)).T
        for k in (2, 1):
            h = 2 - k
            at = slice(h * cr, (h + 1) * cr)
            x = part[c, k, at, :] + precv[c, 2, at, :].astype(jnp.int32).astype(F32) * ucol[at, :1]
            encode(c, k, h, x)
        for k in (2, 1):
            usend[c, k - 1] = col[c, k - 1].T[:8, :]
            go(part_copy(c, k, 2 - k, k, 3 + k))
            go(unit_copy(c, k, 1 + k))

    column = lax.broadcasted_iota(jnp.int32, (cr, width), 1) + v * width
    lane = lax.broadcasted_iota(jnp.int32, (cr, 128), 1)

    def stat_copy(c, k):
        return remote(
            stats.at[c, v], stats.at[c, v], st_send.at[c, k - 1], st_recv.at[c, k - 1],
            {"vocab": lax.rem(v + k, nv)},
        )

    def measure(c):
        for k in (1, 2):
            part_copy(c, k, k - 1, k, 1 + k).wait_recv()
            part_copy(c, k, 2 - k, k, 3 + k).wait_recv()
            unit_copy(c, k, 1 + k).wait_recv()
        row = lax.broadcasted_iota(jnp.int32, (128, count), 0)
        ucol = jnp.where(row == 0, urecv[c, 2][0:1, :], urecv[c, 3][0:1, :]).T
        for h in range(2):
            at = slice(h * cr, (h + 1) * cr)
            natural = slice(h * half + c * cr, h * half + (c + 1) * cr)
            x = part[c, 0, at, :]
            for k in (1, 2):
                x = x + precv[c, k - 1, at, :].astype(jnp.int32).astype(F32) * ucol[at, k - 1:k]
            top = jnp.max(x, axis=1, keepdims=True)
            e = jnp.exp(x - top)
            total = jnp.sum(e, axis=1, keepdims=True)
            pick = jnp.sum(jnp.where(column == tcol[natural, :1], x, 0.0), axis=1, keepdims=True)
            part[c, 0, at, :] = e
            col[c, 0, at, :] = jnp.where(lane == 0, top, jnp.where(lane == 1, total, pick))
        stats[c, v] = col[c, 0].T[:8, :]
        for k in range(1, nv):
            go(stat_copy(c, k))

    def grad_copy(c, k):
        return remote(
            grads.at[c, 0], grads.at[c, k], g_send.at[c, k - 1], g_recv.at[c, k - 1], {"dp": flip(d, k)}
        )

    def differentiate(c):
        own_top = stats[c, v][0:1, :]
        for k in range(1, nv):
            stat_copy(c, k).wait_recv()
        top = stats[c, 0][0:1, :]
        for u in range(1, nv):
            top = jnp.maximum(top, stats[c, u][0:1, :])
        total = jnp.zeros_like(top)
        pick = jnp.zeros_like(top)
        for u in range(nv):
            block = stats[c, u]
            total = total + block[1:2, :] * jnp.exp(block[0:1, :] - top)
            pick = pick + block[2:3, :]
        loss = top + jnp.log(total) - pick
        ratio = jnp.exp(own_top - top) / total
        row = lax.broadcasted_iota(jnp.int32, (128, count), 0)
        both = jnp.where(row == 0, ratio, loss).T
        for h in range(2):
            at = slice(h * cr, (h + 1) * cr)
            natural = slice(h * half + c * cr, h * half + (c + 1) * cr)
            losscol[natural, :] = jnp.broadcast_to(both[at, 1:2], (cr, 128))
            weight = ccol[natural, :1]
            onehot = jnp.where(column == tcol[natural, :1], weight, 0.0)
            g = part[c, 0, at, :] * (both[at, :1] * weight) - onehot
            grads[c, 0, at, :] = g.astype(BF16)
        for k in (1, 2):
            go(grad_copy(c, k))

    def relay_copy(c, k):
        at = pl.ds((k - 1) * cr, cr)
        return remote(
            grads.at[c, k, at], grads.at[c, 3, at], r_send.at[c, k - 1], r_recv.at[c, k - 1], {"dp": flip(d, 3 - k)}
        )

    def relay(c):
        for k in (1, 2):
            grad_copy(c, k).wait_recv()
            go(relay_copy(c, k))

    depth_tile = min(256, depth)
    chunk_rows = min(16, cr)

    def mate_sum(c):
        return remote(xsend.at[c], xrecv.at[c], x_send.at[c], x_recv.at[c], {"vocab": mate})

    def pull(c):
        for k in (1, 2):
            relay_copy(c, k).wait_recv()

        def step(n, _):
            at = pl.ds(pl.multiple_of(n * depth_tile, depth_tile), depth_tile)
            value = lax.dot_general(
                grads[c].reshape(total_rows, width), w[at, :], (((1,), (1,)), ((), ())),
                preferred_element_type=F32,
            )
            acc[c, :, :, :, at] = value.reshape(nd, 2, cr, depth_tile)
            return 0

        lax.fori_loop(0, depth // depth_tile, step, 0)

        def cast(k, _):
            for i in range(cr // chunk_rows):
                at = slice(i * chunk_rows, (i + 1) * chunk_rows)
                xsend[c, k, at, :] = acc[c, k, 1 - core, at, :].astype(BF16)
            return 0

        lax.fori_loop(0, nd, cast, 0)
        go(mate_sum(c))

    far = jnp.where(2 * z < chips, chips - 1, 0)
    near_end = jnp.logical_or(z == 0, z == chips - 1)
    goals = []
    for j in range(chips - 1):
        inner = jnp.where(2 * z < chips, jnp.where(z == 0, chips - 1 - j, (3, 0, 2)[j]), jnp.where(z == chips - 1, j, (0, 3, 1)[j]))
        goals.append(inner)
    goals.append(z)

    def chain_copy(c, j, goal):
        back = jnp.where(goal < z, 1, 0)
        return remote(
            zsend.at[c, j], zrecv.at[back, c, goal], z_send.at[c, j], z_recv.at[back, c, goal],
            {"vocab": v + 2 - 4 * back},
        )

    def each(body):
        def step(i, _):
            body(pl.ds(pl.multiple_of(i * chunk_rows, chunk_rows), chunk_rows))
            return 0

        lax.fori_loop(0, cr // chunk_rows, step, 0)

    def exchange(c):
        mate_sum(c).wait_recv()

    def forward(c, j):
        goal = goals[j]
        k = xor(d, goal)
        back = jnp.where(goal < z, 1, 0)

        @pl.when(near_end)
        def _():
            def first(at):
                zsend[c, j, at, :] = (acc[c, k, core, at, :] + xrecv[c, k, at, :].astype(F32)).astype(BF16)

            each(first)

        @pl.when(jnp.logical_not(near_end))
        def _():
            chain_copy(c, j, goal).wait_recv()

            def add(at):
                zsend[c, j, at, :] = (
                    acc[c, k, core, at, :] + xrecv[c, k, at, :].astype(F32) + zrecv[back, c, goal, at, :].astype(F32)
                ).astype(BF16)

            each(add)

        chain_copy(c, j, goal).start()

    def arrive(c, back):
        return remote(zsend.at[c, 0], zrecv.at[back, c, z], z_send.at[c, 0], z_recv.at[back, c, z], {"vocab": mate})

    def finish(c):
        k = xor(d, z)
        back = jnp.where(z == 0, 1, 0)

        def there(at):
            return pl.ds(pl.multiple_of(c * cr + at.start, chunk_rows), chunk_rows)

        @pl.when(near_end)
        def _():
            arrive(c, back).wait_recv()

            def add(at):
                gh_ref[there(at), :] = (
                    acc[c, k, core, at, :] + xrecv[c, k, at, :].astype(F32) + zrecv[back, c, z, at, :].astype(F32)
                ).astype(BF16)

            each(add)

        @pl.when(jnp.logical_not(near_end))
        def _():
            arrive(c, 0).wait_recv()
            arrive(c, 1).wait_recv()

            def add(at):
                gh_ref[there(at), :] = (
                    acc[c, k, core, at, :] + xrecv[c, k, at, :].astype(F32)
                    + zrecv[0, c, z, at, :].astype(F32) + zrecv[1, c, z, at, :].astype(F32)
                ).astype(BF16)

            each(add)

    def weigh(n):
        at = pl.ds(n * depth_tile, depth_tile)
        gw_ref[at, :] = lax.dot_general(
            spread[:, :, :, at].reshape(chunks * total_rows, depth_tile),
            grads[...].reshape(chunks * total_rows, width),
            (((0,), (0,)), ((), ())), preferred_element_type=F32,
        ).astype(BF16)

    steps = {
        "a": gather, "b": cross, "p": project, "s": scatter, "r": combine, "m": measure, "g": differentiate,
        "l": relay, "u": pull, "x": exchange, "f": finish, "w": weigh,
    }
    for name in plan:
        if name[0] == "y":
            forward(int(name[1]), int(name[2]))
        else:
            steps[name[0]](int(name[1]))

    loss_ref[...] = losscol[...].T[:1, :]
    for copy in sent:
        copy.wait_send()
    for c in range(chunks):
        for j, goal in enumerate(goals[:-1]):
            chain_copy(c, j, goal).wait_send()


PLAN = (
    "a0", "a1", "b0", "a2", "p0", "b1", "s0", "a3", "p1", "r0", "b2", "s1", "p2", "s2",
    "r1", "m0", "r2", "b3", "g0", "p3", "m1", "s3", "m2", "l0", "r3", "g1", "g2", "m3",
    "u0", "l1", "g3", "l2", "x0", "y00", "y01", "y02", "u1", "l3", "u2", "x1", "y10", "u3",
    "x2", "y20", "y11", "x3", "y30", "y12", "w2", "w5", "w7", "w1", "w6", "y21", "w3", "y31",
    "y22", "w4", "f0", "w0", "f1", "y32", "f2", "f3",
)


def chain(nd, nv, hidden, weight, targets, cotangent):
    rows = hidden.shape[0]
    tokens = rows * nd
    depth, width = weight.shape
    share = tokens // nv
    chips = nv // 2
    cr = rows // 2 // CHUNKS
    count = 2 * cr
    dma = pltpu.SemaphoreType.DMA
    vmem = pl.BlockSpec(memory_space=pltpu.VMEM)
    anywhere = pl.BlockSpec(memory_space=pl.ANY)
    flops = 6 * tokens * depth * width

    def both(*shape):
        return [dma(shape), dma(shape)]

    loss, grad_hidden, grad_weight = pl.pallas_call(
        functools.partial(chain_kernel, nd, nv, PLAN),
        out_shape=(
            pltpu.VMEM((1, rows), F32),
            pltpu.VMEM((share, depth), BF16),
            pltpu.VMEM((depth, width), BF16),
        ),
        in_specs=[anywhere, anywhere, vmem, vmem],
        out_specs=(vmem, vmem, vmem),
        scratch_shapes=[
            pltpu.VMEM((depth, width), BF16),
            pltpu.VMEM((CHUNKS, nd, count, depth), BF16),
            pltpu.VMEM((CHUNKS, nd, count, width), F32),
            pltpu.VMEM((CHUNKS, nd - 1, count, width), WIRE),
            pltpu.VMEM((CHUNKS, nd - 1, count, width), WIRE),
            pltpu.VMEM((CHUNKS, nd - 1, 8, count), F32),
            pltpu.VMEM((CHUNKS, 4, 8, count), F32),
            pltpu.VMEM((CHUNKS, nv, 8, count), F32),
            pltpu.VMEM((CHUNKS, nd, count, width), BF16),
            pltpu.VMEM((CHUNKS, nd, 2, cr, depth), F32),
            pltpu.VMEM((CHUNKS, nd, cr, depth), BF16),
            pltpu.VMEM((CHUNKS, nd, cr, depth), BF16),
            pltpu.VMEM((CHUNKS, chips - 1, cr, depth), BF16),
            pltpu.VMEM((2, CHUNKS, chips, cr, depth), BF16),
            pltpu.VMEM((rows, 128), jnp.int32),
            pltpu.VMEM((rows, 128), F32),
            pltpu.VMEM((CHUNKS, nd - 1, count, 128), F32),
            pltpu.VMEM((rows, 128), F32),
            dma, dma((CHUNKS, 2)),
            *both(CHUNKS, nd - 1), *both(CHUNKS), *both(CHUNKS, 2), *both(CHUNKS, 6), *both(CHUNKS, 4),
            *both(CHUNKS, nv - 1), *both(CHUNKS, 2), *both(CHUNKS, 2), *both(CHUNKS),
            dma((CHUNKS, chips - 1)), dma((2, CHUNKS, chips)),
        ],
        compiler_params=pltpu.CompilerParams(
            collective_id=0, has_side_effects=True, vmem_limit_bytes=VMEM_GRANT
        ),
        cost_estimate=pl.CostEstimate(flops=flops, bytes_accessed=16 << 20, transcendentals=0),
        name="token_loss",
    )(hidden, weight, targets.reshape(1, rows), cotangent.reshape(1, rows))
    return loss.reshape(rows), grad_hidden, grad_weight


def solution(mesh):
    in_specs = (P("dp", None), P("dp", "vocab"), P("dp"), P("dp"))
    out_specs = (P("dp"), P("vocab", "dp"), P("dp", "vocab"))
    nd, nv = mesh.shape["dp"], mesh.shape["vocab"]
    form = chain if nd == 4 and nv == 2 * nd else butterfly
    body = functools.partial(form, nd, nv)
    return jax.shard_map(body, mesh=mesh, in_specs=in_specs, out_specs=out_specs, check_vma=False)
```
